32 devices in a mesh: seq: 8 (over z, y), ch: 4 (over x, core).
Axes of the slice: x: 2, y: 2, z: 4, core: 2. Of those that a mesh axis runs over, the one named last changes fastest.
Arguments:
- queries: bfloat16 [2048, 4096], P('seq', 'ch'), may hold values from -6 to 6
- keys: bfloat16 [2048, 4096], P('seq', 'ch'), may hold values from -6 to 6
- values: bfloat16 [2048, 4096], P('seq', 'ch'), may hold values from -6 to 6
- filters: bfloat16 [4096, 2048], P('ch', 'seq'), may hold values from -2 to 2
- skip_gain: float32 [4096], P('ch'), may hold values from 0.5 to 1.5
- projection: bfloat16 [4096, 4096], P(None, 'ch'), may hold values from -0.09375 to 0.09375
Outputs:
- mixed_out: bfloat16 [2048, 4096], P('seq', 'ch')
The draws below stay inside these ranges and needn't reach their ends.
All inputs are finite; a program needn't handle non-finite values.
Results may differ from the reference program's by a relative error of at most 0.006.
Values may be sent and summed in bfloat16 or wider, within the bound.
No kernel may reach another device: no remote copies, remote signals or barrier semaphores. Data moves between devices by JAX's collectives and lax.ppermute only.
A program may use at most 128 MiB of HBM per device.

```python
import jax
import jax.numpy as jnp
from jax import lax

D = 4096
TOKENS = 2048


def draw_filters(key, part):
    key_rate, key_taps = jax.random.split(jax.random.fold_in(key, 11))
    length = TOKENS
    unit = jax.random.uniform(key_rate, (D, 1), jnp.float32)
    lowest = 30.0
    highest = 4.0 * length
    decay_len = lowest * jnp.exp(unit * jnp.log(highest / lowest))
    positions = jnp.arange(length, dtype=jnp.float32)[None, :]
    envelope = jnp.exp(-positions / decay_len)
    norms = jnp.sqrt(jnp.sum(envelope * envelope, axis=1, keepdims=True))
    taps = jax.random.truncated_normal(key_taps, -4.0, 4.0, (D, length), jnp.float32)
    return (taps * envelope / norms).astype(jnp.bfloat16)


def steps_of(stream_key, shape, cuts, least, largest):
    gain = 1.0
    for axis_at, shards_of in cuts:
        draws = jax.random.uniform(jax.random.fold_in(jax.random.fold_in(stream_key, 6), axis_at), (shards_of,), jnp.float32, least / len(cuts), largest / len(cuts))
        gain = gain * jnp.repeat(jnp.exp(draws), shape[axis_at] // shards_of).reshape((-1,) + (1,) * (len(shape) - 1 - axis_at))
    return gain


def normal_values(stream_key, extent, width, bound, pieces=(), kind=jnp.bfloat16):
    array = jax.random.normal(stream_key, extent, jnp.float32) * width
    if len(pieces) > 0:
        array = steps_of(stream_key, extent, pieces, -0.22, 0.18) * array
    return jnp.clip(array, min=-bound, max=bound).astype(kind)


def setup_inputs(seed: int = 0) -> dict:
    streams_of = jax.random.split(jax.random.key(seed), 7)
    queries = normal_values(streams_of[0], (TOKENS, D), 1.0, 6.0, ((0, 8), (1, 4)))
    keys = normal_values(streams_of[1], (TOKENS, D), 1.0, 6.0, ((0, 8), (1, 4)))
    values = normal_values(streams_of[2], (TOKENS, D), 1.0, 6.0, ((0, 8), (1, 4)))
    filters = draw_filters(jax.random.fold_in(streams_of[6], 71), 0)
    skip_gain = jnp.clip(1.0 + 0.1 * jax.random.normal(streams_of[4], (D,), jnp.float32), 0.5, 1.5)
    projection = normal_values(streams_of[5], (D, D), D ** -0.5, 0.09375, ((1, 4),))
    return dict(queries=queries, keys=keys, values=values, filters=filters, skip_gain=skip_gain, projection=projection)


def reference(queries, keys, values, filters, skip_gain, projection):
    gated_kv = (keys.astype(jnp.float32) * values.astype(jnp.float32)).astype(jnp.bfloat16)
    block_width = min(D, 256)
    blocks = D // block_width
    padded_len = 2 * TOKENS
    inputs = gated_kv.astype(jnp.float32).reshape(TOKENS, blocks, block_width).transpose(1, 0, 2)
    kernels = filters.astype(jnp.float32).reshape(blocks, block_width, TOKENS).transpose(0, 2, 1)

    def convolve_block(operands):
        signal, kernel = operands
        product = jnp.fft.rfft(signal, n=padded_len, axis=0) * jnp.fft.rfft(kernel, n=padded_len, axis=0)
        return jnp.fft.irfft(product, n=padded_len, axis=0)[:TOKENS]

    convolved = lax.map(convolve_block, (inputs, kernels))
    convolved = convolved.transpose(1, 0, 2).reshape(TOKENS, D).astype(jnp.bfloat16)
    mixed_in = (queries.astype(jnp.float32) * (convolved.astype(jnp.float32) + skip_gain.astype(jnp.float32)[None, :] * gated_kv.astype(jnp.float32))).astype(jnp.bfloat16)
    return jnp.dot(mixed_in, projection, preferred_element_type=jnp.float32).astype(jnp.bfloat16)
```

```python
import functools
import math

import jax
import jax.numpy as jnp
import numpy as np
from jax import lax
from jax.experimental import pallas as pl
from jax.experimental.pallas import tpu as pltpu
from jax.sharding import PartitionSpec as P


F32 = jnp.float32
BF16 = jnp.bfloat16
LANES = 128
INNER = 128
ROWS = 16
CORES = 4


def cmul(a, w):
    re, im = a
    c, s = float(w.real), float(w.imag)
    if abs(s) < 1e-12:
        return (re, im) if abs(c - 1) < 1e-12 else (re * c, im * c)
    if abs(c) < 1e-12:
        return (-im, re) if s > 0 else (im, -re)
    if abs(abs(c) - abs(s)) < 1e-12:
        h = abs(c)
        if c > 0 and s < 0:
            return ((re + im) * h, (im - re) * h)
        if c > 0:
            return ((re - im) * h, (im + re) * h)
        if s < 0:
            return ((im - re) * h, (re + im) * -h)
        return ((re + im) * -h, (re - im) * h)
    return (re * c - im * s, re * s + im * c)


def root(size, index, sign):
    return complex(np.exp(sign * 2j * np.pi * (index % size) / size))


def complex_dft(z, sign):
    size = len(z)
    if size == 1:
        return z
    half = size // 2
    low = [(z[i][0] + z[i + half][0], z[i][1] + z[i + half][1]) for i in range(half)]
    high = [
        cmul((z[i][0] - z[i + half][0], z[i][1] - z[i + half][1]), root(size, i, sign))
        for i in range(half)
    ]
    even, odd = complex_dft(low, sign), complex_dft(high, sign)
    return [even[i // 2] if i % 2 == 0 else odd[i // 2] for i in range(size)]


def odd_dft(x):
    size = len(x)
    if size == 1:
        return {1: (x[0], None)}
    half = size // 2
    z = [cmul((x[i], -x[i + half]), root(2 * size, i, -1)) for i in range(half)]
    out = {}
    for p, (re, im) in enumerate(complex_dft(z, -1)):
        freq = 4 * p + 1
        if freq <= size:
            out[freq] = (re, im)
        else:
            out[2 * size - freq] = (re, -im)
    return out


def real_dft(x):
    size = len(x)
    if size == 1:
        return {0: (x[0], None)}
    half = size // 2
    out = {2 * k: v for k, v in real_dft([x[i] + x[i + half] for i in range(half)]).items()}
    out.update(odd_dft([x[i] - x[i + half] for i in range(half)]))
    return out


def padded_dft(x):
    out = {2 * k: v for k, v in real_dft(x).items()}
    out.update(odd_dft(x))
    return out


def odd_adjoint(t, size):
    if size == 1:
        return [t[1][0]]
    half = size // 2
    z = []
    for p in range(half):
        freq = 4 * p + 1
        if freq <= size:
            z.append(t[freq])
        else:
            re, im = t[2 * size - freq]
            z.append((re, -im))
    z = complex_dft(z, 1)
    z = [cmul(z[i], root(2 * size, i, 1)) for i in range(half)]
    return [v[0] for v in z] + [-v[1] for v in z]


def real_adjoint(t, size):
    if size == 1:
        return [t[0][0]]
    half = size // 2
    even = real_adjoint({k // 2: v for k, v in t.items() if k % 2 == 0}, half)
    odd = odd_adjoint({k: v for k, v in t.items() if k % 2 == 1}, half)
    return [even[i] + odd[i] for i in range(half)] + [even[i] - odd[i] for i in range(half)]


def padded_adjoint(t, size):
    even = real_adjoint({k // 2: v for k, v in t.items() if k % 2 == 0}, size)
    odd = odd_adjoint({k: v for k, v in t.items() if k % 2 == 1}, size)
    return [even[i] + odd[i] for i in range(size)]


def split_np(table):
    high = table.astype(BF16)
    return high, (table - high.astype(np.float64)).astype(BF16)


def make_tables(outer):
    size = 2 * outer * INNER
    at = np.outer(np.arange(INNER), np.arange(INNER)) % INNER
    cos = np.cos(2 * np.pi * at / INNER)
    sin = np.sin(2 * np.pi * at / INNER)
    forward = np.block([[cos, sin], [-sin, cos]])
    backward = np.block([[cos, -sin], [sin, cos]]) / size
    at = np.outer(np.arange(outer + 1), np.arange(INNER)) * (2 * np.pi / size)
    turn = np.stack([np.cos(at), np.sin(at)], 1).astype(np.float32)
    turn = np.broadcast_to(turn[..., None], turn.shape + (LANES,))
    return split_np(forward), split_np(backward), np.ascontiguousarray(turn)


def split(value):
    high = value.astype(BF16)
    return high, (value - high.astype(F32)).astype(BF16)


def dot(a, b):
    return jnp.dot(a, b, preferred_element_type=F32)


def dot3(table_hi, table_lo, data_hi, data_lo):
    return dot(table_hi, data_hi) + (dot(table_lo, data_hi) + dot(table_hi, data_lo))


def outer_forward(planes, turn, data_hi, data_lo, outer):
    def block(index, carry):
        at = pl.ds(pl.multiple_of(index * ROWS, ROWS), ROWS)
        under = pl.ds(pl.multiple_of(INNER + index * ROWS, ROWS), ROWS)
        spectrum = padded_dft([planes[i, at, :].astype(F32) for i in range(outer)])
        for k in range(outer + 1):
            re, im = spectrum[k]
            c, s = turn[k, 0, at, :], turn[k, 1, at, :]
            if k == 0:
                im = jnp.zeros_like(re)
            elif im is None:
                re, im = re * c, -(re * s)
            else:
                re, im = re * c + im * s, im * c - re * s
            lanes = pl.ds((k % 2) * LANES, LANES)
            for rows, value in ((at, re), (under, im)):
                high, low = split(value)
                data_hi[k // 2, rows, lanes] = high
                data_lo[k // 2, rows, lanes] = low
        return carry

    lax.fori_loop(0, INNER // ROWS, block, 0)


def pair_width(pair, outer):
    return LANES if 2 * pair + 1 > outer else 2 * LANES


def spectrum_kernel(groups, outer, *refs):
    blocks = refs[:groups]
    turn, hi, lo, out, planes, data_hi, data_lo = refs[groups:]
    me = lax.axis_index("seq")
    per = outer // groups
    for j in range(groups):
        source = lax.bitwise_xor(me, j)
        for i in range(per):
            taps = blocks[j][:, i * INNER : (i + 1) * INNER].astype(F32)
            planes[source * per + i] = taps.T.astype(BF16)
    outer_forward(planes, turn, data_hi, data_lo, outer)
    for pair in range(outer // 2 + 1):
        width = pair_width(pair, outer)
        out[pair, :, :width] = dot3(
            hi[...], lo[...], data_hi[pair, :, :width], data_lo[pair, :, :width]
        )


def convolve_kernel(groups, outer, *refs):
    blocks = refs[:groups]
    turn, hi, lo, back_hi, back_lo, kernel_spec = refs[groups : groups + 6]
    outs = refs[groups + 6 : 2 * groups + 6]
    planes, data_hi, data_lo, turned, result = refs[2 * groups + 6 :]
    me = lax.axis_index("seq")
    per = outer // groups
    for j in range(groups):
        source = lax.bitwise_xor(me, j)
        for i in range(per):
            planes[source * per + i] = blocks[j][i * INNER : (i + 1) * INNER, :]
    outer_forward(planes, turn, data_hi, data_lo, outer)
    for pair in range(outer // 2 + 1):
        width = pair_width(pair, outer)
        spec = dot3(hi[...], lo[...], data_hi[pair, :, :width], data_lo[pair, :, :width])
        re, im = spec[:INNER], spec[INNER:]
        k_re, k_im = kernel_spec[pair, :INNER, :width], kernel_spec[pair, INNER:, :width]
        product = jnp.concatenate([re * k_re - im * k_im, re * k_im + im * k_re], 0)
        high, low = split(product)
        turned[pair, :, :width] = dot3(back_hi[...], back_lo[...], high, low)

    def block(index, carry):
        at = pl.ds(pl.multiple_of(index * ROWS, ROWS), ROWS)
        under = pl.ds(pl.multiple_of(INNER + index * ROWS, ROWS), ROWS)
        spectrum = {}
        for k in range(outer + 1):
            lanes = pl.ds((k % 2) * LANES, LANES)
            re, im = turned[k // 2, at, lanes], turned[k // 2, under, lanes]
            c, s = turn[k, 0, at, :], turn[k, 1, at, :]
            if k == 0:
                spectrum[k] = (re, None)
            elif k == outer:
                spectrum[k] = (re * c - im * s, None)
            else:
                spectrum[k] = (2 * (re * c - im * s), 2 * (im * c + re * s))
        for i, value in enumerate(padded_adjoint(spectrum, outer)):
            result[i, at, :] = value.astype(BF16)
        return carry

    lax.fori_loop(0, INNER // ROWS, block, 0)
    for j in range(groups):
        target = lax.bitwise_xor(me, j)
        for i in range(per):
            outs[j][i * INNER : (i + 1) * INNER, :] = result[target * per + i]


def gate_in_kernel(groups, keys, values, *outs):
    me = lax.axis_index("seq")
    for j in range(groups):
        at = pl.ds(pl.multiple_of(lax.bitwise_xor(me, j) * LANES, LANES), LANES)
        outs[j][...] = (keys[:, at].astype(F32) * values[:, at].astype(F32)).astype(BF16)


def cut_kernel(groups, filters, *outs):
    me = lax.axis_index("seq")
    for j in range(groups):
        at = pl.ds(pl.multiple_of(lax.bitwise_xor(me, j) * LANES, LANES), LANES)
        outs[j][...] = filters[at, :]


def gate_out_kernel(first, count, *refs):
    convolved, gated = refs[:count], refs[count : 2 * count]
    queries, gain, out = refs[2 * count :]
    me = lax.axis_index("seq")
    for j in range(count):
        group = lax.bitwise_xor(me, first + j)
        at = pl.ds(pl.multiple_of(group * LANES, LANES), LANES)
        to = pl.ds(pl.multiple_of(lax.rem(group, count) * LANES, LANES), LANES)
        mixed = queries[:, at].astype(F32) * (
            convolved[j][...].astype(F32) + gain[:, at] * gated[j][...].astype(F32)
        )
        out[:, to] = mixed.astype(BF16)


def project_kernel(count, last, index_ref, *refs):
    mixed, weights = refs[:count], refs[count : 2 * count]
    total = None
    if last:
        total = refs[2 * count][...]
    out = refs[-1]
    for a, b in zip(mixed, weights):
        part = dot(a[...], b[...])
        total = part if total is None else total + part
    out[...] = total.astype(out.dtype)


VMEM = pl.BlockSpec(memory_space=pltpu.VMEM)


def call(kernel, name, out_shape, args, scratch=(), limit=None, flops=1_000_000, moved=1_000_000):
    many = isinstance(out_shape, (list, tuple))
    return pl.pallas_call(
        kernel,
        name=name,
        out_shape=out_shape,
        in_specs=[VMEM] * len(args),
        out_specs=[VMEM] * len(out_shape) if many else VMEM,
        scratch_shapes=list(scratch),
        compiler_params=pltpu.CompilerParams(vmem_limit_bytes=limit),
        cost_estimate=pl.CostEstimate(flops=flops, bytes_accessed=moved, transcendentals=0),
    )(*args)


def project(mixed, rows, projection, total, dtype):
    count = len(mixed)
    tokens, depth = mixed[0].shape
    width = projection.shape[1]
    tile = min(256, width)
    index = jnp.stack([r.astype(jnp.int32) for r in rows])
    in_specs = [pl.BlockSpec((tokens, depth), lambda n, at: (0, 0)) for _ in range(count)]
    in_specs += [
        pl.BlockSpec((depth, tile), functools.partial(lambda i, n, at: (at[i], n), i))
        for i in range(count)
    ]
    args = list(mixed) + [projection] * count
    if total is not None:
        in_specs.append(pl.BlockSpec((tokens, tile), lambda n, at: (0, n)))
        args.append(total)
    return pl.pallas_call(
        functools.partial(project_kernel, count, total is not None),
        name="project",
        grid_spec=pltpu.PrefetchScalarGridSpec(
            num_scalar_prefetch=1,
            grid=(width // tile,),
            in_specs=in_specs,
            out_specs=pl.BlockSpec((tokens, tile), lambda n, at: (0, n)),
        ),
        out_shape=jax.ShapeDtypeStruct((tokens, width), dtype),
        compiler_params=pltpu.CompilerParams(vmem_limit_bytes=20 << 20),
        cost_estimate=pl.CostEstimate(
            flops=2 * tokens * depth * width * count,
            bytes_accessed=2 * depth * width * count,
            transcendentals=0,
        ),
    )(index, *args)


def swap(block, axis, size, mask):
    return lax.ppermute(block, axis, [(i, i ^ mask) for i in range(size)])


def send_order(groups):
    return sorted(range(1, groups), key=lambda j: -j)


def exchange(blocks, groups):
    arrived = [blocks[0]] + [None] * (groups - 1)
    for j in send_order(groups):
        arrived[j] = swap(blocks[j], "seq", groups, j)
    return arrived


def fast(queries, keys, values, filters, skip_gain, projection):
    tokens, width = queries.shape
    groups = lax.axis_size("seq")
    outer = tokens * groups // INNER
    pairs = outer // 2 + 1
    (hi, lo), (back_hi, back_lo), turn = make_tables(outer)
    block = jax.ShapeDtypeStruct((tokens, LANES), BF16)
    taps = call(
        functools.partial(cut_kernel, groups),
        "cut",
        [jax.ShapeDtypeStruct((LANES, tokens), BF16)] * groups,
        [filters],
        limit=4 << 20,
    )
    taps = exchange(taps, groups)
    gated = call(
        functools.partial(gate_in_kernel, groups), "gate_in", [block] * groups, [keys, values],
        limit=6 << 20,
    )
    signals = exchange(gated, groups)
    scratch = [
        pltpu.VMEM((outer, INNER, LANES), BF16),
        pltpu.VMEM((pairs, 2 * INNER, 2 * LANES), BF16),
        pltpu.VMEM((pairs, 2 * INNER, 2 * LANES), BF16),
    ]
    flops = 3 * 2 * pairs * (2 * INNER) ** 2 * 2 * LANES
    spec = call(
        functools.partial(spectrum_kernel, groups, outer),
        "spectrum",
        jax.ShapeDtypeStruct((pairs, 2 * INNER, 2 * LANES), F32),
        list(taps) + [turn, hi, lo],
        scratch,
        limit=20 << 20,
        flops=flops,
    )
    convolved = call(
        functools.partial(convolve_kernel, groups, outer),
        "convolve",
        [block] * groups,
        list(signals) + [turn, hi, lo, back_hi, back_lo, spec],
        scratch
        + [
            pltpu.VMEM((pairs, 2 * INNER, 2 * LANES), F32),
            pltpu.VMEM((outer, INNER, LANES), BF16),
        ],
        limit=24 << 20,
        flops=2 * flops,
    )
    convolved = exchange(convolved, groups)
    half = groups // 2
    me = lax.axis_index("seq")
    mine = lax.axis_index("ch")
    gain = skip_gain[None, :]
    total = None
    for part in range(2):
        some = slice(part * half, (part + 1) * half)
        mixed = call(
            functools.partial(gate_out_kernel, part * half, half),
            "gate_out",
            jax.ShapeDtypeStruct((tokens, width // 2), BF16),
            list(convolved[some]) + list(gated[some]) + [queries, gain],
            limit=8 << 20,
        )
        far = swap(mixed, "ch", CORES, 2)
        near = swap(mixed, "ch", CORES, 1)
        relayed = swap(far, "ch", CORES, 1)
        side = lax.bitwise_xor(me // half, part)
        rows = [lax.bitwise_xor(mine, j) * 2 + side for j in range(CORES)]
        total = project(
            [mixed, near, far, relayed], rows, projection, total, F32 if part == 0 else BF16
        )
    return total


table_precision = lax.Precision.HIGH


def make_table(row_count, col_count, modulus):
    product = (
        jnp.arange(row_count, dtype=jnp.int32)[:, None]
        * jnp.arange(col_count, dtype=jnp.int32)[None, :]
        % modulus
    )
    angles = product.astype(jnp.float32) * (-2.0 * math.pi / modulus)
    return (jnp.cos(angles), jnp.sin(angles))


def transform_tables(length):
    padded_len = 2 * length
    factor_a = 1
    for attempt in range(40):
        if factor_a * factor_a * 4 <= padded_len and length % (factor_a * 2) == 0:
            factor_a = factor_a * 2
    factor_b = padded_len // factor_a
    half_b = factor_b // 2
    outer_table = make_table(factor_b, half_b, factor_b)
    inner_table = make_table(factor_a, factor_a, factor_a)
    twiddle = make_table(factor_b, factor_a, padded_len)
    return (outer_table, inner_table, twiddle, factor_a, half_b, padded_len)


def forward_spectrum(signal, tables):
    outer_table, inner_table, twiddle, factor_a, half_b, padded_len = tables
    chan_count = signal.shape[0]
    shaped = signal.reshape(chan_count, half_b, factor_a)
    section_re = jnp.einsum("kh,cha->cka", outer_table[0], shaped, precision=table_precision)
    section_im = jnp.einsum("kh,cha->cka", outer_table[1], shaped, precision=table_precision)
    turned_re = section_re * twiddle[0] - section_im * twiddle[1]
    turned_im = section_re * twiddle[1] + section_im * twiddle[0]
    spec_re = jnp.dot(turned_re, inner_table[0], precision=table_precision) - jnp.dot(
        turned_im, inner_table[1], precision=table_precision
    )
    spec_im = jnp.dot(turned_re, inner_table[1], precision=table_precision) + jnp.dot(
        turned_im, inner_table[0], precision=table_precision
    )
    return (spec_re, spec_im)


def causal_convolve(signal, kernel_spec, tables):
    outer_table, inner_table, twiddle, factor_a, half_b, padded_len = tables
    chan_count = signal.shape[0]
    sig_re, sig_im = forward_spectrum(signal, tables)
    prod_re = sig_re * kernel_spec[0] - sig_im * kernel_spec[1]
    prod_im = sig_re * kernel_spec[1] + sig_im * kernel_spec[0]
    back_re = jnp.dot(prod_re, inner_table[0], precision=table_precision) + jnp.dot(
        prod_im, inner_table[1], precision=table_precision
    )
    back_im = jnp.dot(prod_im, inner_table[0], precision=table_precision) - jnp.dot(
        prod_re, inner_table[1], precision=table_precision
    )
    turned_re = back_re * twiddle[0] + back_im * twiddle[1]
    turned_im = back_im * twiddle[0] - back_re * twiddle[1]
    real_part = jnp.einsum("kh,cka->cha", outer_table[0], turned_re, precision=table_precision)
    real_part = real_part + jnp.einsum(
        "kh,cka->cha", outer_table[1], turned_im, precision=table_precision
    )
    return (real_part / padded_len).reshape(chan_count, half_b * factor_a)


def return_tokens(convolved):
    packed = convolved.astype(jnp.bfloat16)[None]
    return lax.all_to_all(packed, "seq", split_axis=2, concat_axis=0, tiled=True)


def plain(queries, keys, values, filters, skip_gain, projection):
    token_count, chan_width = queries.shape
    groups = lax.axis_size("seq")
    per_group = chan_width // groups
    length = token_count * groups
    tables = transform_tables(length)
    gated_kv = (keys.astype(jnp.float32) * values.astype(jnp.float32)).astype(jnp.bfloat16)
    kv_blocks = gated_kv.T.reshape(groups, per_group, token_count)
    tap_blocks = filters.reshape(groups, per_group, token_count)
    signals = lax.all_to_all(kv_blocks, "seq", split_axis=0, concat_axis=2, tiled=True)
    kernels = lax.all_to_all(tap_blocks, "seq", split_axis=0, concat_axis=2, tiled=True)
    kernel_spec = forward_spectrum(kernels[0].astype(jnp.float32), tables)
    convolved = return_tokens(causal_convolve(signals[0].astype(jnp.float32), kernel_spec, tables))
    convolved = convolved.reshape(chan_width, token_count)
    mixed_in = (
        queries.T.astype(jnp.float32)
        * (convolved.astype(jnp.float32) + skip_gain[:, None] * gated_kv.T.astype(jnp.float32))
    ).astype(jnp.bfloat16)
    mixed_out = lax.dot_general(
        lax.all_gather(mixed_in, "ch", axis=0, tiled=True),
        projection,
        (((0,), (0,)), ((), ())),
        preferred_element_type=jnp.float32,
    )
    return mixed_out.astype(jnp.bfloat16)


def on_device(queries, *rest):
    tokens, width = queries.shape
    groups = lax.axis_size("seq")
    fits = (
        width == groups * LANES
        and tokens % INNER == 0
        and groups >= 2
        and groups & (groups - 1) == 0
        and (tokens // INNER) & (tokens // INNER - 1) == 0
        and tokens * groups <= 32 * INNER
        and lax.axis_size("ch") == CORES
    )
    return (fast if fits else plain)(queries, *rest)


def solution(mesh):
    return jax.shard_map(
        on_device,
        mesh=mesh,
        in_specs=(
            P("seq", "ch"),
            P("seq", "ch"),
            P("seq", "ch"),
            P("ch", "seq"),
            P("ch"),
            P(None, "ch"),
        ),
        out_specs=P("seq", "ch"),
        check_vma=False,
    )
```

```python
import functools
import math

import jax
import jax.numpy as jnp
import numpy as np
from jax import lax
from jax.experimental import pallas as pl
from jax.experimental.pallas import tpu as pltpu
from jax.sharding import PartitionSpec as P


F32 = jnp.float32
BF16 = jnp.bfloat16
LANES = 128
INNER = 128
ROWS = 16
CORES = 4


def cmul(a, w):
    re, im = a
    c, s = float(w.real), float(w.imag)
    if abs(s) < 1e-12:
        return (re, im) if abs(c - 1) < 1e-12 else (re * c, im * c)
    if abs(c) < 1e-12:
        return (-im, re) if s > 0 else (im, -re)
    if abs(abs(c) - abs(s)) < 1e-12:
        h = abs(c)
        if c > 0 and s < 0:
            return ((re + im) * h, (im - re) * h)
        if c > 0:
            return ((re - im) * h, (im + re) * h)
        if s < 0:
            return ((im - re) * h, (re + im) * -h)
        return ((re + im) * -h, (re - im) * h)
    return (re * c - im * s, re * s + im * c)


def root(size, index, sign):
    return complex(np.exp(sign * 2j * np.pi * (index % size) / size))


def complex_dft(z, sign):
    size = len(z)
    if size == 1:
        return z
    half = size // 2
    low = [(z[i][0] + z[i + half][0], z[i][1] + z[i + half][1]) for i in range(half)]
    high = [
        cmul((z[i][0] - z[i + half][0], z[i][1] - z[i + half][1]), root(size, i, sign))
        for i in range(half)
    ]
    even, odd = complex_dft(low, sign), complex_dft(high, sign)
    return [even[i // 2] if i % 2 == 0 else odd[i // 2] for i in range(size)]


def odd_dft(x):
    size = len(x)
    if size == 1:
        return {1: (x[0], None)}
    half = size // 2
    z = [cmul((x[i], -x[i + half]), root(2 * size, i, -1)) for i in range(half)]
    out = {}
    for p, (re, im) in enumerate(complex_dft(z, -1)):
        freq = 4 * p + 1
        if freq <= size:
            out[freq] = (re, im)
        else:
            out[2 * size - freq] = (re, -im)
    return out


def real_dft(x):
    size = len(x)
    if size == 1:
        return {0: (x[0], None)}
    half = size // 2
    out = {2 * k: v for k, v in real_dft([x[i] + x[i + half] for i in range(half)]).items()}
    out.update(odd_dft([x[i] - x[i + half] for i in range(half)]))
    return out


def padded_dft(x):
    out = {2 * k: v for k, v in real_dft(x).items()}
    out.update(odd_dft(x))
    return out


def odd_adjoint(t, size):
    if size == 1:
        return [t[1][0]]
    half = size // 2
    z = []
    for p in range(half):
        freq = 4 * p + 1
        if freq <= size:
            z.append(t[freq])
        else:
            re, im = t[2 * size - freq]
            z.append((re, -im))
    z = complex_dft(z, 1)
    z = [cmul(z[i], root(2 * size, i, 1)) for i in range(half)]
    return [v[0] for v in z] + [-v[1] for v in z]


def real_adjoint(t, size):
    if size == 1:
        return [t[0][0]]
    half = size // 2
    even = real_adjoint({k // 2: v for k, v in t.items() if k % 2 == 0}, half)
    odd = odd_adjoint({k: v for k, v in t.items() if k % 2 == 1}, half)
    return [even[i] + odd[i] for i in range(half)] + [even[i] - odd[i] for i in range(half)]


def padded_adjoint(t, size):
    even = real_adjoint({k // 2: v for k, v in t.items() if k % 2 == 0}, size)
    odd = odd_adjoint({k: v for k, v in t.items() if k % 2 == 1}, size)
    return [even[i] + odd[i] for i in range(size)]


def split_np(table):
    high = table.astype(BF16)
    return high, (table - high.astype(np.float64)).astype(BF16)


def make_tables(outer):
    size = 2 * outer * INNER
    at = np.outer(np.arange(INNER), np.arange(INNER)) % INNER
    cos = np.cos(2 * np.pi * at / INNER)
    sin = np.sin(2 * np.pi * at / INNER)
    forward = np.block([[cos, sin], [-sin, cos]])
    backward = np.block([[cos, -sin], [sin, cos]]) / size
    at = np.outer(np.arange(outer + 1), np.arange(INNER)) * (2 * np.pi / size)
    turn = np.stack([np.cos(at), np.sin(at)], 1).astype(np.float32)
    turn = np.broadcast_to(turn[..., None], turn.shape + (LANES,))
    return split_np(forward), split_np(backward), np.ascontiguousarray(turn)


def split(value):
    high = value.astype(BF16)
    return high, (value - high.astype(F32)).astype(BF16)


def dot(a, b):
    return jnp.dot(a, b, preferred_element_type=F32)


def dot3(table_hi, table_lo, data_hi, data_lo):
    return dot(table_hi, data_hi) + (dot(table_lo, data_hi) + dot(table_hi, data_lo))


def outer_forward(planes, turn, data_hi, data_lo, outer):
    def block(index, carry):
        at = pl.ds(pl.multiple_of(index * ROWS, ROWS), ROWS)
        under = pl.ds(pl.multiple_of(INNER + index * ROWS, ROWS), ROWS)
        spectrum = padded_dft([planes[i, at, :].astype(F32) for i in range(outer)])
        for k in range(outer + 1):
            re, im = spectrum[k]
            c, s = turn[k, 0, at, :], turn[k, 1, at, :]
            if k == 0:
                im = jnp.zeros_like(re)
            elif im is None:
                re, im = re * c, -(re * s)
            else:
                re, im = re * c + im * s, im * c - re * s
            lanes = pl.ds((k % 2) * LANES, LANES)
            for rows, value in ((at, re), (under, im)):
                high, low = split(value)
                data_hi[k // 2, rows, lanes] = high
                data_lo[k // 2, rows, lanes] = low
        return carry

    lax.fori_loop(0, INNER // ROWS, block, 0)


def pair_width(pair, outer):
    return LANES if 2 * pair + 1 > outer else 2 * LANES


def spectrum_kernel(groups, outer, *refs):
    blocks = refs[:groups]
    turn, hi, lo, out, planes, data_hi, data_lo = refs[groups:]
    me = lax.axis_index("seq")
    per = outer // groups
    for j in range(groups):
        source = lax.bitwise_xor(me, j)
        for i in range(per):
            taps = blocks[j][i * LANES : (i + 1) * LANES, :].astype(F32)
            planes[source * per + i] = taps.T.astype(BF16)
    outer_forward(planes, turn, data_hi, data_lo, outer)
    for pair in range(outer // 2 + 1):
        width = pair_width(pair, outer)
        out[pair, :, :width] = dot3(
            hi[...], lo[...], data_hi[pair, :, :width], data_lo[pair, :, :width]
        )


def convolve_kernel(groups, outer, *refs):
    blocks = refs[:groups]
    turn, hi, lo, back_hi, back_lo, kernel_spec = refs[groups : groups + 6]
    outs = refs[groups + 6 : 2 * groups + 6]
    planes, data_hi, data_lo, turned, result = refs[2 * groups + 6 :]
    me = lax.axis_index("seq")
    per = outer // groups
    for j in range(groups):
        source = lax.bitwise_xor(me, j)
        skip = per * INNER if j < groups // 2 else 0
        for i in range(per):
            first = skip + i * INNER
            planes[source * per + i] = blocks[j][first : first + INNER, :]
    outer_forward(planes, turn, data_hi, data_lo, outer)
    for pair in range(outer // 2 + 1):
        width = pair_width(pair, outer)
        spec = dot3(hi[...], lo[...], data_hi[pair, :, :width], data_lo[pair, :, :width])
        re, im = spec[:INNER], spec[INNER:]
        k_re, k_im = kernel_spec[pair, :INNER, :width], kernel_spec[pair, INNER:, :width]
        product = jnp.concatenate([re * k_re - im * k_im, re * k_im + im * k_re], 0)
        high, low = split(product)
        turned[pair, :, :width] = dot3(back_hi[...], back_lo[...], high, low)

    def block(index, carry):
        at = pl.ds(pl.multiple_of(index * ROWS, ROWS), ROWS)
        under = pl.ds(pl.multiple_of(INNER + index * ROWS, ROWS), ROWS)
        spectrum = {}
        for k in range(outer + 1):
            lanes = pl.ds((k % 2) * LANES, LANES)
            re, im = turned[k // 2, at, lanes], turned[k // 2, under, lanes]
            c, s = turn[k, 0, at, :], turn[k, 1, at, :]
            if k == 0:
                spectrum[k] = (re, None)
            elif k == outer:
                spectrum[k] = (re * c - im * s, None)
            else:
                spectrum[k] = (2 * (re * c - im * s), 2 * (im * c + re * s))
        for i, value in enumerate(padded_adjoint(spectrum, outer)):
            result[i, at, :] = value.astype(BF16)
        return carry

    lax.fori_loop(0, INNER // ROWS, block, 0)
    for j in range(groups):
        target = lax.bitwise_xor(me, j)
        for i in range(per):
            outs[j][i * INNER : (i + 1) * INNER, :] = result[target * per + i]


def cut_kernel(groups, filters, *outs):
    me = lax.axis_index("seq")
    tokens = filters.shape[1]
    for j in range(groups):
        at = pl.ds(pl.multiple_of(lax.bitwise_xor(me, j) * LANES, LANES), LANES)
        for i in range(0, tokens, LANES):
            outs[j][i : i + LANES, :] = filters[at, i : i + LANES]


def gate_in_kernel(groups, *refs):
    half = groups // 2
    near_taps, (keys, values) = refs[:half], refs[half : half + 2]
    near, far = refs[half + 2 : groups + 2], refs[groups + 2 :]
    me = lax.axis_index("seq")
    tokens = keys.shape[0]
    for j in range(groups):
        at = pl.ds(pl.multiple_of(lax.bitwise_xor(me, j) * LANES, LANES), LANES)
        product = (keys[:, at].astype(F32) * values[:, at].astype(F32)).astype(BF16)
        if j < half:
            near[j][:tokens, :] = near_taps[j][...]
            near[j][tokens:, :] = product
        else:
            far[j - half][...] = product


def gate_out_kernel(first, count, *refs):
    convolved, gated = refs[:count], refs[count : 2 * count]
    queries, gain, out = refs[2 * count :]
    me = lax.axis_index("seq")
    tokens = out.shape[0]
    for j in range(count):
        group = lax.bitwise_xor(me, first + j)
        at = pl.ds(pl.multiple_of(group * LANES, LANES), LANES)
        to = pl.ds(pl.multiple_of(lax.rem(group, count) * LANES, LANES), LANES)
        signal = gated[j][gated[j].shape[0] - tokens :, :]
        mixed = queries[:, at].astype(F32) * (
            convolved[j][...].astype(F32) + gain[:, at] * signal.astype(F32)
        )
        out[:, to] = mixed.astype(BF16)


def products(mixed, weights, out, total=None):
    width = out.shape[1]
    tile = min(256, width)
    for n in range(0, width, tile):
        at = slice(n, n + tile)
        value = None if total is None else total[:, at]
        for a, b in zip(mixed, weights):
            part = dot(a[...], b[:, at])
            value = part if value is None else value + part
        out[:, at] = value.astype(out.dtype)


def project_kernel(part, first, count, start, *refs):
    mixed, projection = refs[:count], refs[count]
    total = None if start else refs[count + 1]
    depth = mixed[0].shape[1]
    side = lax.axis_index("seq") // (lax.axis_size("seq") // 2)
    mine = lax.axis_index("ch")
    weights = []
    for j in range(first, first + count):
        row = (lax.bitwise_xor(mine, j) * 2 + lax.bitwise_xor(side, part)) * depth
        weights.append(projection.at[pl.ds(pl.multiple_of(row, depth), depth), :])
    products(mixed, weights, refs[-1], total)


VMEM = pl.BlockSpec(memory_space=pltpu.VMEM)


def call(kernel, out_shape, args, scratch=(), limit=None, flops=1_000_000):
    many = isinstance(out_shape, (list, tuple))
    result = pl.pallas_call(
        kernel,
        out_shape=out_shape,
        in_specs=[VMEM] * len(args),
        out_specs=[VMEM] * len(out_shape) if many else VMEM,
        scratch_shapes=list(scratch),
        compiler_params=pltpu.CompilerParams(vmem_limit_bytes=limit),
        cost_estimate=pl.CostEstimate(flops=flops, bytes_accessed=1_000_000, transcendentals=0),
    )(*args)
    return list(result) if many else result


def swap(block, axis, size, mask):
    return lax.ppermute(block, axis, [(i, i ^ mask) for i in range(size)])


def array(*shape, dtype=BF16):
    return jax.ShapeDtypeStruct(shape, dtype)


def fast(queries, keys, values, filters, skip_gain, projection):
    return fast_body(queries, keys, values, filters, skip_gain, projection)


def fast_body(queries, keys, values, filters, skip_gain, projection):
    tokens, width = queries.shape
    groups = lax.axis_size("seq")
    half = groups // 2
    outer = tokens * groups // INNER
    pairs = outer // 2 + 1
    (hi, lo), (back_hi, back_lo), turn = make_tables(outer)
    taps = call(
        functools.partial(cut_kernel, groups), [array(tokens, LANES)] * groups, [filters],
        limit=2 << 20,
        flops=5_000_000_000,
    )
    entered = call(
        functools.partial(gate_in_kernel, groups),
        [array(2 * tokens, LANES)] * half + [array(tokens, LANES)] * half,
        taps[:half] + [keys, values],
        limit=4 << 20,
        flops=5_000_000_000,
    )
    near, far_signals = entered[:half], entered[half:]
    far_taps = [swap(taps[j], "seq", groups, j) for j in range(half, groups)]
    signals = [swap(b, "seq", groups, half + j) for j, b in enumerate(far_signals)]
    both = [near[0]] + [swap(near[j], "seq", groups, j) for j in range(1, half)]
    gated = list(near) + list(far_signals)
    scratch = [
        pltpu.VMEM((outer, INNER, LANES), BF16),
        pltpu.VMEM((pairs, 2 * INNER, 2 * LANES), BF16),
        pltpu.VMEM((pairs, 2 * INNER, 2 * LANES), BF16),
    ]
    flops = 3 * 2 * pairs * (2 * INNER) ** 2 * 2 * LANES
    spec = call(
        functools.partial(spectrum_kernel, groups, outer),
        array(pairs, 2 * INNER, 2 * LANES, dtype=F32),
        both + far_taps + [turn, hi, lo],
        scratch,
        limit=20 << 20,
        flops=flops,
    )
    convolved = call(
        functools.partial(convolve_kernel, groups, outer),
        [array(tokens, LANES)] * groups,
        both + signals + [turn, hi, lo, back_hi, back_lo, spec],
        scratch
        + [
            pltpu.VMEM((pairs, 2 * INNER, 2 * LANES), F32),
            pltpu.VMEM((outer, INNER, LANES), BF16),
        ],
        limit=24 << 20,
        flops=2 * flops,
    )
    convolved = [convolved[0]] + [swap(convolved[j], "seq", groups, j) for j in range(1, groups)]
    gain = skip_gain[None, :]
    blocks = []
    for part in range(2):
        some = slice(part * half, (part + 1) * half)
        mixed = call(
            functools.partial(gate_out_kernel, part * half, half),
            array(tokens, width // 2),
            convolved[some] + gated[some] + [queries, gain],
            limit=8 << 20,
        )
        far = swap(mixed, "ch", CORES, 2)
        near = swap(mixed, "ch", CORES, 1)
        relayed = swap(far, "ch", CORES, 1)
        blocks.append([mixed, near, far, relayed])
    columns = projection.shape[1]
    depth = width // 2
    total = []
    for name, part, first, count in (("early", 0, 0, 4), ("more", 1, 0, 3), ("last", 1, 3, 1)):
        total = [
            call(
                functools.partial(project_kernel, part, first, count, not total),
                array(tokens, columns, dtype=BF16 if name == "last" else F32),
                blocks[part][first : first + count] + [projection] + total,
                limit=4 << 20,
                flops=2 * count * tokens * depth * columns,
            )
        ]
    return total[0]


table_precision = lax.Precision.HIGH


def make_table(row_count, col_count, modulus):
    product = (
        jnp.arange(row_count, dtype=jnp.int32)[:, None]
        * jnp.arange(col_count, dtype=jnp.int32)[None, :]
        % modulus
    )
    angles = product.astype(jnp.float32) * (-2.0 * math.pi / modulus)
    return (jnp.cos(angles), jnp.sin(angles))


def transform_tables(length):
    padded_len = 2 * length
    factor_a = 1
    for _ in range(40):
        if factor_a * factor_a * 4 <= padded_len and length % (factor_a * 2) == 0:
            factor_a = factor_a * 2
    factor_b = padded_len // factor_a
    half_b = factor_b // 2
    outer_table = make_table(factor_b, half_b, factor_b)
    inner_table = make_table(factor_a, factor_a, factor_a)
    twiddle = make_table(factor_b, factor_a, padded_len)
    return (outer_table, inner_table, twiddle, factor_a, half_b, padded_len)


def forward_spectrum(signal, tables):
    outer_table, inner_table, twiddle, factor_a, half_b, _ = tables
    chan_count = signal.shape[0]
    shaped = signal.reshape(chan_count, half_b, factor_a)
    section_re = jnp.einsum("kh,cha->cka", outer_table[0], shaped, precision=table_precision)
    section_im = jnp.einsum("kh,cha->cka", outer_table[1], shaped, precision=table_precision)
    turned_re = section_re * twiddle[0] - section_im * twiddle[1]
    turned_im = section_re * twiddle[1] + section_im * twiddle[0]
    spec_re = jnp.dot(turned_re, inner_table[0], precision=table_precision) - jnp.dot(
        turned_im, inner_table[1], precision=table_precision
    )
    spec_im = jnp.dot(turned_re, inner_table[1], precision=table_precision) + jnp.dot(
        turned_im, inner_table[0], precision=table_precision
    )
    return (spec_re, spec_im)


def causal_convolve(signal, kernel_spec, tables):
    outer_table, inner_table, twiddle, factor_a, half_b, padded_len = tables
    chan_count = signal.shape[0]
    sig_re, sig_im = forward_spectrum(signal, tables)
    prod_re = sig_re * kernel_spec[0] - sig_im * kernel_spec[1]
    prod_im = sig_re * kernel_spec[1] + sig_im * kernel_spec[0]
    back_re = jnp.dot(prod_re, inner_table[0], precision=table_precision) + jnp.dot(
        prod_im, inner_table[1], precision=table_precision
    )
    back_im = jnp.dot(prod_im, inner_table[0], precision=table_precision) - jnp.dot(
        prod_re, inner_table[1], precision=table_precision
    )
    turned_re = back_re * twiddle[0] + back_im * twiddle[1]
    turned_im = back_im * twiddle[0] - back_re * twiddle[1]
    real_part = jnp.einsum("kh,cka->cha", outer_table[0], turned_re, precision=table_precision)
    real_part = real_part + jnp.einsum(
        "kh,cka->cha", outer_table[1], turned_im, precision=table_precision
    )
    return (real_part / padded_len).reshape(chan_count, half_b * factor_a)


def return_tokens(convolved):
    packed = convolved.astype(jnp.bfloat16)[None]
    return lax.all_to_all(packed, "seq", split_axis=2, concat_axis=0, tiled=True)


def plain(queries, keys, values, filters, skip_gain, projection):
    token_count, chan_width = queries.shape
    groups = lax.axis_size("seq")
    per_group = chan_width // groups
    length = token_count * groups
    tables = transform_tables(length)
    gated_kv = (keys.astype(jnp.float32) * values.astype(jnp.float32)).astype(jnp.bfloat16)
    kv_blocks = gated_kv.T.reshape(groups, per_group, token_count)
    tap_blocks = filters.reshape(groups, per_group, token_count)
    signals = lax.all_to_all(kv_blocks, "seq", split_axis=0, concat_axis=2, tiled=True)
    kernels = lax.all_to_all(tap_blocks, "seq", split_axis=0, concat_axis=2, tiled=True)
    kernel_spec = forward_spectrum(kernels[0].astype(jnp.float32), tables)
    convolved = return_tokens(causal_convolve(signals[0].astype(jnp.float32), kernel_spec, tables))
    convolved = convolved.reshape(chan_width, token_count)
    mixed_in = (
        queries.T.astype(jnp.float32)
        * (convolved.astype(jnp.float32) + skip_gain[:, None] * gated_kv.T.astype(jnp.float32))
    ).astype(jnp.bfloat16)
    mixed_out = lax.dot_general(
        lax.all_gather(mixed_in, "ch", axis=0, tiled=True),
        projection,
        (((0,), (0,)), ((), ())),
        preferred_element_type=jnp.float32,
    )
    return mixed_out.astype(jnp.bfloat16)


def on_device(queries, *rest):
    tokens, width = queries.shape
    groups = lax.axis_size("seq")
    projection_rows = rest[-1].shape[0]
    fits = (
        width == groups * LANES
        and tokens % INNER == 0
        and projection_rows == width * CORES
        and groups >= 2
        and groups & (groups - 1) == 0
        and (tokens // INNER) & (tokens // INNER - 1) == 0
        and tokens * groups <= 32 * INNER
        and lax.axis_size("ch") == CORES
    )
    return (fast if fits else plain)(queries, *rest)


def solution(mesh):
    return jax.shard_map(
        on_device,
        mesh=mesh,
        in_specs=(
            P("seq", "ch"),
            P("seq", "ch"),
            P("seq", "ch"),
            P("ch", "seq"),
            P("ch"),
            P(None, "ch"),
        ),
        out_specs=P("seq", "ch"),
        check_vma=False,
    )
```
